32 devices in a mesh: expert: 4 (over y, core), shard: 8 (over z, x).
Axes of the slice: x: 2, y: 2, z: 4, core: 2. Of those that a mesh axis runs over, the one named last changes fastest.
Arguments:
- w_gate: float32 [128, 2048, 768], P('expert', 'shard'), may hold values from -0.1875 to 0.1875
- w_up: float32 [128, 2048, 768], P('expert', 'shard'), may hold values from -0.1875 to 0.1875
- router_weight: float32 [2048, 128], P('shard', 'expert'), may hold values from -0.125 to 0.125
- router_gain: float32 [2048], P('shard'), may hold values from 0.25 to 1.75
Outputs:
- serve_gate: bfloat16 [128, 2048, 768], P('expert', None, 'shard')
- serve_up: bfloat16 [128, 2048, 768], P('expert', None, 'shard')
- scale_gate: float32 [128, 768], P('expert', 'shard')
- scale_up: float32 [128, 768], P('expert', 'shard')
- serve_router: bfloat16 [2048, 128], replicated
The draws below stay inside these ranges and needn't reach their ends.
All inputs are finite; a program needn't handle non-finite values. Where the reference program divides by a largest or mean magnitude, that divisor is 1e-20 or more.
Results may differ from the reference program's by a relative error of at most 0.001.
Values may be sent and summed in bfloat16 or wider, within the bound.
A program may use at most 192 MiB of HBM per device.

```python
import jax
import jax.numpy as jnp

EXPERTS = 128
D_MODEL = 2048
D_EXPERT = 768


def with_spikes(result, stream_key, source, target, blocks, factor):
    def block_of(dim):
        return (jnp.arange(result.shape[dim]) // (result.shape[dim] // blocks)).reshape((-1,) + (1,) * (result.ndim - 1 - dim))

    near = jax.random.permutation(stream_key, blocks)[block_of(target)]
    other_side = (block_of(target) + blocks // 2) % blocks
    return jnp.where((block_of(source) == near) | (block_of(source) == other_side), factor * result, result)


def block_levels(rng, shape, cuts, low, largest):
    loudness, own = 1.0, jax.random.fold_in(rng, 6)
    for dim, blocks in cuts:
        steps = jnp.exp(jax.random.uniform(jax.random.fold_in(own, dim), (blocks,), jnp.float32, low / len(cuts), largest / len(cuts)))
        loudness = loudness * jnp.repeat(steps, shape[dim] // blocks).reshape([-1 if axis == dim else 1 for axis in range(len(shape))])
    return loudness


def normal_values(key, shape, deviation, reach, split=(), kind=jnp.bfloat16):
    loudness = block_levels(key, shape, split, -0.22, 0.18) if split else 1.0
    result = jax.random.normal(key, shape, jnp.float32) * deviation * loudness
    return jnp.minimum(jnp.maximum(result, -reach), reach).astype(kind)


def bell_draw_with(key, dims, width, most, cuts, heavy, dtype=jnp.bfloat16):
    result = width * jax.random.normal(key, dims, jnp.float32)
    if cuts:
        result = result * block_levels(key, dims, cuts, -0.22, 0.18)
    return jnp.clip(with_spikes(result, jax.random.fold_in(key, 3), *heavy), -most, most).astype(dtype)


def setup_inputs(seed: int = 0) -> dict:
    arg_keys = jax.random.split(jax.random.key(seed), 5)
    w_gate = bell_draw_with(arg_keys[0], (EXPERTS, D_MODEL, D_EXPERT), D_MODEL ** -0.5, 0.1875, ((0, 4), (1, 8)), (1, 2, 8, 2.0), jnp.float32)
    w_up = bell_draw_with(arg_keys[1], (EXPERTS, D_MODEL, D_EXPERT), D_MODEL ** -0.5, 0.1875, ((0, 4), (1, 8)), (1, 2, 8, 2.0), jnp.float32)
    router_weight = normal_values(arg_keys[2], (D_MODEL, EXPERTS), D_MODEL ** -0.5, 0.125, ((0, 8), (1, 4)), jnp.float32)
    router_gain = jnp.clip(1.0 + 0.15 * jax.random.normal(arg_keys[3], (D_MODEL,), jnp.float32), 0.25, 1.75)
    return dict(w_gate=w_gate, w_up=w_up, router_weight=router_weight, router_gain=router_gain)


def reference(w_gate, w_up, router_weight, router_gain):
    scale_gate = jnp.max(jnp.abs(w_gate), axis=1)
    serve_gate = (w_gate / jnp.expand_dims(scale_gate, 1)).astype(jnp.bfloat16)
    scale_up = jnp.max(jnp.abs(w_up), axis=1)
    serve_up = (w_up / jnp.expand_dims(scale_up, 1)).astype(jnp.bfloat16)
    serve_router = (router_weight * router_gain[:, None]).astype(jnp.bfloat16)
    return serve_gate, serve_up, scale_gate, scale_up, serve_router
```

```python
import functools

import jax
import jax.numpy as jnp
from jax import lax
from jax.experimental import pallas as pl
from jax.experimental.pallas import tpu as pltpu
from jax.sharding import PartitionSpec as P

MESH = pl.DeviceIdType.MESH
SLOTS = 8
LANES = 128
NOW = 2
DIRECT = 8
EARLY = 3
CHUNK = 4


def kernel(
    n, ne,
    gate, up, router, gain,
    serve, out_scale, out_router,
    gm, ring, send, lmax, dbuf, rsbuf, half_max, xbuf, rbuf,
    load_sem, send_sem, recv_sem,
    d_send, d_recv, rs_send, rs_recv, x_send, x_recv, ag_send, ag_recv,
    r0_send, r0_recv, r1_send, r1_recv, r2_send, r2_recv,
):
    me = lax.axis_index("shard")
    my_e = lax.axis_index("expert")
    experts, rows, cols = gate.shape
    part = cols // n
    total = 2 * experts
    h = n // 2
    mine = lax.rem(me, h)
    base = me - mine
    far = (n - h) - base
    share = (total - DIRECT) // h
    peers = range(n - 1)

    def there(l):
        if l < h:
            return far + lax.rem(mine + l, h)
        return base + lax.rem(mine + (l - h + 1), h)

    def back(l):
        if l < h:
            return far + lax.rem(mine + (h - l), h)
        return base + lax.rem(mine + (2 * h - 1 - l), h)

    def near(s):
        return base + lax.rem(mine + s, h)

    def near_back(s):
        return base + lax.rem(mine + (h - s), h)

    def remote(src, dst, ssem, rsem, device):
        return pltpu.make_async_remote_copy(
            src_ref=src, dst_ref=dst, send_sem=ssem, recv_sem=rsem,
            device_id=device, device_id_type=MESH,
        )

    def load(array, index, slot):
        return pltpu.make_async_copy(array.at[index], ring.at[slot], load_sem.at[slot])

    def item_of(k):
        early = jnp.where(k < DIRECT, k, k - DIRECT)
        late = jnp.where(k < total + EARLY, k - EARLY, k - total)
        return jnp.where(k < DIRECT + EARLY, early, late)

    def fetch(k):
        slot = lax.rem(k, SLOTS)
        item = item_of(k)

        @pl.when((k < 2 * total) & (item < experts))
        def _():
            load(gate, item, slot).start()

        @pl.when((k < 2 * total) & (item >= experts))
        def _():
            load(up, item - experts, slot).start()

    for k in range(SLOTS):
        load((gate, up)[k // experts], k % experts, k).start()

    barrier = pltpu.get_barrier_semaphore()
    for l in peers:
        pl.semaphore_signal(barrier, inc=1, device_id={"shard": there(l)}, device_id_type=MESH)
    for r in range(1, ne):
        pl.semaphore_signal(
            barrier, inc=1, device_id={"expert": lax.rem(my_e + r, ne)}, device_id_type=MESH
        )

    def direct(b, l, slot):
        first, count = ((0, NOW), (NOW, DIRECT - NOW))[b]
        return remote(
            lmax.at[pl.ds(first, count)], dbuf.at[slot, pl.ds(first, count)],
            d_send.at[b, l], d_recv.at[b, l], {"shard": there(l)},
        )

    def spread(s, slot):
        return remote(
            lmax.at[pl.ds(DIRECT + lax.rem(mine + s, h) * share, share)], rsbuf.at[s],
            rs_send.at[s], rs_recv.at[s], {"shard": near(s)},
        )

    def swap():
        return remote(half_max, xbuf, x_send, x_recv, {"shard": far + mine})

    def collect(s, slot):
        block = pl.ds(DIRECT + slot * share, share)
        return remote(gm.at[block], gm.at[block], ag_send.at[s], ag_recv.at[s], {"shard": near(s)})

    def router_swap(slot):
        return remote(
            rbuf.at[my_e, me], rbuf.at[my_e, slot], r0_send, r0_recv, {"shard": far + mine}
        )

    def router_row(s, j, slot):
        return remote(
            rbuf.at[my_e, slot], rbuf.at[my_e, slot],
            r1_send.at[s, j], r1_recv.at[s, j], {"shard": near(s)},
        )

    def router_col(r, slot):
        return remote(
            rbuf.at[slot], rbuf.at[slot], r2_send.at[r], r2_recv.at[r],
            {"expert": lax.rem(my_e + r, ne)},
        )

    def column(slot):
        return pl.ds(pl.multiple_of(slot * rows, LANES), rows)

    def peer_rows(slot):
        return pl.ds(pl.multiple_of(slot * part, 16), part)

    def piece(l, slot, first, count):
        return remote(
            send.at[pl.ds(first, count), peer_rows(there(l))],
            serve.at[pl.ds(first, count), :, column(slot)],
            send_sem.at[l], recv_sem.at[l], {"shard": there(l)},
        )

    def maxima(k, item):
        slot = lax.rem(k, SLOTS)
        load(gate, 0, slot).wait()
        lmax[item] = jnp.max(jnp.abs(ring[slot]), axis=0, keepdims=True)
        fetch(k + SLOTS)

    def quotient(k, item):
        slot = lax.rem(k, SLOTS)
        load(gate, 0, slot).wait()
        inverse = 1.0 / gm[item]
        for j in range(0, cols, LANES):
            block = ring[slot, :, j:j + LANES] * inverse[:, j:j + LANES]
            send[item, j:j + LANES, :] = block.T.astype(jnp.bfloat16)
        fetch(k + SLOTS)
        serve[item, :, column(me)] = send[item, peer_rows(me), :]

    def ship(first, count):
        for l in peers:
            piece(l, me, first, count).start()

    def settle(b):
        first, count = ((0, NOW), (NOW, DIRECT - NOW))[b]
        span = pl.ds(first, count)
        largest = lmax[span]
        for l in peers:
            direct(b, l, back(l)).wait_recv()
            largest = jnp.maximum(largest, dbuf[back(l), span])
        gm[span] = largest

    def maxima_span(first, last, shift):
        @pl.loop(first, last)
        def _(item):
            maxima(item + shift, item)

    def quotient_span(first, last, shift):
        @pl.loop(first, last)
        def _(item):
            quotient(item + shift, item)
            ship(item, 1)

    maxima_span(0, NOW, 0)
    rbuf[my_e, me] = (router[...] * gain[...]).astype(jnp.bfloat16)
    pl.semaphore_wait(barrier, n + ne - 2)
    for l in peers:
        direct(0, l, me).start()
    router_swap(me).start()
    maxima_span(NOW, DIRECT, 0)
    for l in peers:
        direct(1, l, me).start()
    settle(0)
    quotient_span(0, NOW, DIRECT)
    settle(1)
    quotient_span(NOW, EARLY, DIRECT)
    maxima_span(DIRECT, total, EARLY)

    for s in range(1, h):
        spread(s, mine).start()
    quotient_span(EARLY, EARLY + 1, total)
    largest = lmax[pl.ds(DIRECT + mine * share, share)]
    for s in range(1, h):
        spread(s, mine).wait_recv()
        largest = jnp.maximum(largest, rsbuf[s])
    half_max[...] = largest
    router_swap(far + mine).wait_recv()
    swap().start()
    for s in range(1, h):
        router_row(s, 0, me).start()
        router_row(s, 1, far + mine).start()
    quotient_span(EARLY + 1, EARLY + 2, total)
    swap().wait_recv()
    gm[pl.ds(DIRECT + mine * share, share)] = jnp.maximum(half_max[...], xbuf[...])
    quotient_span(EARLY + 2, EARLY + 3, total)
    for s in range(1, h):
        collect(s, mine).start()
    quotient_span(EARLY + 3, DIRECT, total)
    for s in range(1, h):
        collect(s, lax.rem(mine + (h - s), h)).wait_recv()

    @pl.loop(0, (total - DIRECT) // CHUNK)
    def _(c):
        first = DIRECT + c * CHUNK

        @pl.loop(0, CHUNK)
        def _(i):
            quotient(total + first + i, first + i)

        @pl.when(c > 0)
        def _():
            ship(first - CHUNK, CHUNK)

    ship(total - CHUNK, CHUNK)

    for s in range(1, h):
        router_row(s, 0, near_back(s)).wait_recv()
        router_row(s, 1, far + lax.rem(mine + (h - s), h)).wait_recv()
    for r in range(1, ne):
        router_col(r, my_e).start()
    whole = gm[...].reshape(total, cols)
    for s in range(n):
        @pl.when(me == s)
        def _():
            out_scale[...] = whole[:, s * part:(s + 1) * part]
    for r in range(1, ne):
        router_col(r, lax.rem(my_e + (ne - r), ne)).wait_recv()
    for s in range(n):
        block = rbuf[:, s].astype(jnp.float32).reshape(ne * rbuf.shape[2], rows)
        out_router[s * rows:(s + 1) * rows, :] = block.T.astype(jnp.bfloat16)

    for l in peers:
        for b in range(2):
            direct(b, l, me).wait_send()
    for s in range(1, h):
        spread(s, mine).wait_send()
        collect(s, mine).wait_send()
        router_row(s, 0, me).wait_send()
        router_row(s, 1, far + mine).wait_send()
    swap().wait_send()
    router_swap(me).wait_send()
    for r in range(1, ne):
        router_col(r, my_e).wait_send()
    for l in peers:
        piece(l, me, 0, total).wait_send()
    for l in peers:
        piece(l, back(l), 0, total).wait_recv()


def place(serve, scale, router, out_gate, out_up, out_sg, out_su, out_router, sems):
    experts = out_gate.shape[0]
    moves = (
        (serve.at[pl.ds(0, experts)], out_gate),
        (serve.at[pl.ds(experts, experts)], out_up),
        (router, out_router),
        (scale.at[pl.ds(0, experts)], out_sg),
        (scale.at[pl.ds(experts, experts)], out_su),
    )
    copies = [pltpu.make_async_copy(a, b, sems.at[i]) for i, (a, b) in enumerate(moves)]
    for copy in copies:
        copy.start()
    for copy in copies:
        copy.wait()


def plain_body(w_gate, w_up, router_weight, router_gain):
    scale_gate, scale_up = lax.pmax(
        (jnp.max(jnp.abs(w_gate), axis=1), jnp.max(jnp.abs(w_up), axis=1)), "shard"
    )
    narrow_gate, narrow_up = (
        (w_gate / jnp.expand_dims(scale_gate, 1)).astype(jnp.bfloat16),
        (w_up / jnp.expand_dims(scale_up, 1)).astype(jnp.bfloat16),
    )
    serve_gate, serve_up = (
        lax.all_to_all(narrow_gate, "shard", split_axis=2, concat_axis=1, tiled=True),
        lax.all_to_all(narrow_up, "shard", split_axis=2, concat_axis=1, tiled=True),
    )
    scale_gate = lax.dynamic_slice_in_dim(
        scale_gate, lax.axis_index("shard") * serve_gate.shape[2], serve_gate.shape[2], axis=1
    )
    scale_up = lax.dynamic_slice_in_dim(
        scale_up, lax.axis_index("shard") * serve_up.shape[2], serve_up.shape[2], axis=1
    )
    part_router = (router_weight * router_gain[:, None]).astype(jnp.bfloat16)
    row_router = lax.all_gather(part_router, "shard", axis=0, tiled=True)
    serve_router = lax.all_gather(row_router, "expert", axis=1, tiled=True)
    return (serve_gate, serve_up, scale_gate, scale_up, serve_router)


def body(n, ne, w_gate, w_up, router_weight, router_gain):
    experts, rows, cols = w_gate.shape
    total, h = 2 * experts, n // 2
    fits = (
        n % 2 == 0 and rows % LANES == 0 and cols % LANES == 0 and (cols // n) % 16 == 0
        and total > DIRECT and (total - DIRECT) % h == 0 and (total - DIRECT) % CHUNK == 0
        and total >= SLOTS
    )
    if not fits:
        return plain_body(w_gate, w_up, router_weight, router_gain)
    part, share, local_e = cols // n, (total - DIRECT) // h, router_weight.shape[1]
    dma = pltpu.SemaphoreType.DMA
    anywhere = pl.BlockSpec(memory_space=pl.ANY)
    local = pl.BlockSpec(memory_space=pltpu.VMEM)
    serve, scale, router = pl.pallas_call(
        functools.partial(kernel, n, ne),
        out_shape=(
            pltpu.VMEM((total, part, n * rows), jnp.bfloat16),
            pltpu.VMEM((total, part), jnp.float32),
            pltpu.VMEM((n * rows, ne * local_e), jnp.bfloat16),
        ),
        in_specs=[anywhere, anywhere, local, local],
        out_specs=(local, local, local),
        scratch_shapes=[
            pltpu.VMEM((total, 1, cols), jnp.float32),
            pltpu.VMEM((SLOTS, rows, cols), jnp.float32),
            pltpu.VMEM((total, cols, rows), jnp.bfloat16),
            pltpu.VMEM((total, 1, cols), jnp.float32),
            pltpu.VMEM((n, DIRECT, 1, cols), jnp.float32),
            pltpu.VMEM((h, share, 1, cols), jnp.float32),
            pltpu.VMEM((share, 1, cols), jnp.float32),
            pltpu.VMEM((share, 1, cols), jnp.float32),
            pltpu.VMEM((ne, n, local_e, rows), jnp.bfloat16),
            dma((SLOTS,)),
            dma((n,)),
            dma((n,)),
            dma((2, n)),
            dma((2, n)),
            dma((h,)),
            dma((h,)),
            dma,
            dma,
            dma((h,)),
            dma((h,)),
            dma,
            dma,
            dma((h, 2)),
            dma((h, 2)),
            dma((ne,)),
            dma((ne,)),
        ],
        compiler_params=pltpu.CompilerParams(
            collective_id=0, has_side_effects=True, vmem_limit_bytes=34 * 2**20
        ),
        cost_estimate=pl.CostEstimate(
            flops=4 * experts * rows * cols, bytes_accessed=20 * experts * rows * cols, transcendentals=0
        ),
    )(w_gate, w_up, router_weight.T, router_gain[None, :])
    gate, up, scale_gate, scale_up, router = pl.pallas_call(
        place,
        out_shape=(
            pltpu.HBM((experts, part, n * rows), jnp.bfloat16),
            pltpu.HBM((experts, part, n * rows), jnp.bfloat16),
            pltpu.HBM((experts, part), jnp.float32),
            pltpu.HBM((experts, part), jnp.float32),
            pltpu.HBM((n * rows, ne * local_e), jnp.bfloat16),
        ),
        in_specs=[local] * 3,
        out_specs=(anywhere,) * 5,
        scratch_shapes=[dma((5,))],
        compiler_params=pltpu.CompilerParams(vmem_limit_bytes=2**20),
        cost_estimate=pl.CostEstimate(
            flops=0, bytes_accessed=4 * experts * rows * cols, transcendentals=0
        ),
    )(serve, scale, router)
    return (jnp.swapaxes(gate, 1, 2), jnp.swapaxes(up, 1, 2), scale_gate, scale_up, router)


def solution(mesh):
    return jax.shard_map(
        functools.partial(body, mesh.shape["shard"], mesh.shape["expert"]),
        mesh=mesh,
        in_specs=(
            P("expert", "shard", None),
            P("expert", "shard", None),
            P("shard", "expert"),
            P("shard"),
        ),
        out_specs=(
            P("expert", None, "shard"),
            P("expert", None, "shard"),
            P("expert", "shard"),
            P("expert", "shard"),
            P(),
        ),
        check_vma=False,
    )
```

```python
import functools

import jax
import jax.numpy as jnp
from jax import lax
from jax.experimental import pallas as pl
from jax.experimental.pallas import tpu as pltpu
from jax.sharding import PartitionSpec as P

MESH = pl.DeviceIdType.MESH
SLOTS = 8
LANES = 128
NOW = 2
DIRECT = 8
EARLY = 3
CHUNK = 2
PLACES = 8


def kernel(
    n, ne,
    gate, up, router, gain,
    serve, out_scale, out_router,
    gm, ring, send, lmax, dbuf, rsbuf, half_max, xbuf, rbuf,
    load_sem, send_sem, recv_sem,
    d_send, d_recv, rs_send, rs_recv, x_send, x_recv, ag_send, ag_recv,
    r0_send, r0_recv, r1_send, r1_recv, r2_send, r2_recv,
):
    me = lax.axis_index("shard")
    my_e = lax.axis_index("expert")
    experts, rows, cols = gate.shape
    part = cols // n
    total = 2 * experts
    h = n // 2
    mine = lax.rem(me, h)
    base = me - mine
    far = (n - h) - base
    share = (total - DIRECT) // h
    peers = range(n - 1)

    def there(l):
        if l < h:
            return far + lax.rem(mine + l, h)
        return base + lax.rem(mine + (l - h + 1), h)

    def back(l):
        if l < h:
            return far + lax.rem(mine + (h - l), h)
        return base + lax.rem(mine + (2 * h - 1 - l), h)

    def near(s):
        return base + lax.rem(mine + s, h)

    def near_back(s):
        return base + lax.rem(mine + (h - s), h)

    def remote(src, dst, ssem, rsem, device):
        return pltpu.make_async_remote_copy(
            src_ref=src, dst_ref=dst, send_sem=ssem, recv_sem=rsem,
            device_id=device, device_id_type=MESH,
        )

    def load(array, index, slot):
        return pltpu.make_async_copy(array.at[index], ring.at[slot], load_sem.at[slot])

    def item_of(k):
        early = jnp.where(k < DIRECT, k, k - DIRECT)
        late = jnp.where(k < total + EARLY, k - EARLY, k - total)
        return jnp.where(k < DIRECT + EARLY, early, late)

    def fetch(k):
        slot = lax.rem(k, SLOTS)
        item = item_of(k)

        @pl.when((k < 2 * total) & (item < experts))
        def _():
            load(gate, item, slot).start()

        @pl.when((k < 2 * total) & (item >= experts))
        def _():
            load(up, item - experts, slot).start()

    for k in range(SLOTS):
        load((gate, up)[k // experts], k % experts, k).start()

    barrier = pltpu.get_barrier_semaphore()
    for l in peers:
        pl.semaphore_signal(barrier, inc=1, device_id={"shard": there(l)}, device_id_type=MESH)
    for r in range(1, ne):
        pl.semaphore_signal(
            barrier, inc=1, device_id={"expert": lax.rem(my_e + r, ne)}, device_id_type=MESH
        )

    def direct(b, l, slot):
        first, count = ((0, NOW), (NOW, DIRECT - NOW))[b]
        return remote(
            lmax.at[pl.ds(first, count)], dbuf.at[slot, pl.ds(first, count)],
            d_send.at[b, l], d_recv.at[b, l], {"shard": there(l)},
        )

    def spread(s, slot):
        return remote(
            lmax.at[pl.ds(DIRECT + lax.rem(mine + s, h) * share, share)], rsbuf.at[s],
            rs_send.at[s], rs_recv.at[s], {"shard": near(s)},
        )

    def swap():
        return remote(half_max, xbuf, x_send, x_recv, {"shard": far + mine})

    def collect(s, slot):
        block = pl.ds(DIRECT + slot * share, share)
        return remote(gm.at[block], gm.at[block], ag_send.at[s], ag_recv.at[s], {"shard": near(s)})

    def router_swap(slot):
        return remote(
            rbuf.at[my_e, me], rbuf.at[my_e, slot], r0_send, r0_recv, {"shard": far + mine}
        )

    def router_row(s, j, slot):
        return remote(
            rbuf.at[my_e, slot], rbuf.at[my_e, slot],
            r1_send.at[s, j], r1_recv.at[s, j], {"shard": near(s)},
        )

    def router_col(r, slot):
        return remote(
            rbuf.at[slot], rbuf.at[slot], r2_send.at[r], r2_recv.at[r],
            {"expert": lax.rem(my_e + r, ne)},
        )

    def column(slot):
        return pl.ds(pl.multiple_of(slot * rows, LANES), rows)

    def peer_rows(slot):
        return pl.ds(pl.multiple_of(slot * part, 16), part)

    def piece(l, slot, first, count):
        return remote(
            send.at[pl.ds(first, count), peer_rows(there(l))],
            serve.at[pl.ds(first, count), :, column(slot)],
            send_sem.at[l], recv_sem.at[l], {"shard": there(l)},
        )

    def maxima(k, item):
        slot = lax.rem(k, SLOTS)
        load(gate, 0, slot).wait()
        lmax[item] = jnp.max(jnp.abs(ring[slot]), axis=0, keepdims=True)
        fetch(k + SLOTS)

    def quotient(k, item):
        slot = lax.rem(k, SLOTS)
        load(gate, 0, slot).wait()
        inverse = 1.0 / gm[item]
        for j in range(0, cols, LANES):
            block = ring[slot, :, j:j + LANES] * inverse[:, j:j + LANES]
            send[item, j:j + LANES, :] = block.T.astype(jnp.bfloat16)
        fetch(k + SLOTS)
        serve[item, :, column(me)] = send[item, peer_rows(me), :]

    def ship(first, count):
        for l in sorted(peers, key=lambda l: (l % h, l // h)):
            piece(l, me, first, count).start()

    def settle(b):
        first, count = ((0, NOW), (NOW, DIRECT - NOW))[b]
        span = pl.ds(first, count)
        largest = lmax[span]
        for l in peers:
            direct(b, l, back(l)).wait_recv()
            largest = jnp.maximum(largest, dbuf[back(l), span])
        gm[span] = largest

    def maxima_span(first, last, shift):
        @pl.loop(first, last)
        def _(item):
            maxima(item + shift, item)

    def quotient_span(first, last, shift):
        @pl.loop(first, last)
        def _(item):
            quotient(item + shift, item)
            ship(item, 1)

    maxima_span(0, NOW, 0)
    rbuf[my_e, me] = (router[...] * gain[...]).astype(jnp.bfloat16)
    pl.semaphore_wait(barrier, n + ne - 2)
    for l in peers:
        direct(0, l, me).start()
    router_swap(me).start()
    maxima_span(NOW, DIRECT, 0)
    for l in peers:
        direct(1, l, me).start()
    settle(0)
    quotient_span(0, NOW, DIRECT)
    settle(1)
    quotient_span(NOW, EARLY, DIRECT)
    maxima_span(DIRECT, total, EARLY)

    for s in range(1, h):
        spread(s, mine).start()
    quotient_span(EARLY, EARLY + 1, total)
    largest = lmax[pl.ds(DIRECT + mine * share, share)]
    for s in range(1, h):
        spread(s, mine).wait_recv()
        largest = jnp.maximum(largest, rsbuf[s])
    half_max[...] = largest
    router_swap(far + mine).wait_recv()
    swap().start()
    for s in range(1, h):
        router_row(s, 0, me).start()
        router_row(s, 1, far + mine).start()
    quotient_span(EARLY + 1, EARLY + 2, total)
    swap().wait_recv()
    gm[pl.ds(DIRECT + mine * share, share)] = jnp.maximum(half_max[...], xbuf[...])
    quotient_span(EARLY + 2, EARLY + 3, total)
    for s in range(1, h):
        collect(s, mine).start()
    quotient_span(EARLY + 3, DIRECT, total)
    for s in range(1, h):
        collect(s, lax.rem(mine + (h - s), h)).wait_recv()

    @pl.loop(0, (total - DIRECT) // CHUNK)
    def _(c):
        first = DIRECT + c * CHUNK

        @pl.loop(0, CHUNK)
        def _(i):
            quotient(total + first + i, first + i)

        @pl.when(c > 0)
        def _():
            ship(first - CHUNK, CHUNK)

    ship(total - CHUNK, CHUNK)

    for s in range(1, h):
        router_row(s, 0, near_back(s)).wait_recv()
        router_row(s, 1, far + lax.rem(mine + (h - s), h)).wait_recv()
    for r in range(1, ne):
        router_col(r, my_e).start()
    whole = gm[...].reshape(total, cols)
    for s in range(n):
        @pl.when(me == s)
        def _():
            out_scale[...] = whole[:, s * part:(s + 1) * part]
    for r in range(1, ne):
        router_col(r, lax.rem(my_e + (ne - r), ne)).wait_recv()
    for s in range(n):
        block = rbuf[:, s].astype(jnp.float32).reshape(ne * rbuf.shape[2], rows)
        out_router[s * rows:(s + 1) * rows, :] = block.T.astype(jnp.bfloat16)

    for l in peers:
        for b in range(2):
            direct(b, l, me).wait_send()
    for s in range(1, h):
        spread(s, mine).wait_send()
        collect(s, mine).wait_send()
        router_row(s, 0, me).wait_send()
        router_row(s, 1, far + mine).wait_send()
    swap().wait_send()
    router_swap(me).wait_send()
    for r in range(1, ne):
        router_col(r, my_e).wait_send()
    for l in peers:
        piece(l, me, 0, total).wait_send()
    for l in peers:
        piece(l, back(l), 0, total).wait_recv()


def place(serve, scale, router, out_gate, out_up, out_sg, out_su, out_router, sems):
    experts = out_gate.shape[0]
    step = experts // PLACES
    moves = [
        (serve.at[pl.ds(a * experts + i * step, step)], out.at[pl.ds(i * step, step)])
        for a, out in enumerate((out_gate, out_up))
        for i in range(PLACES)
    ]
    moves += [
        (router, out_router),
        (scale.at[pl.ds(0, experts)], out_sg),
        (scale.at[pl.ds(experts, experts)], out_su),
    ]
    copies = [pltpu.make_async_copy(a, b, sems.at[i]) for i, (a, b) in enumerate(moves)]
    for copy in copies:
        copy.start()
    for copy in copies:
        copy.wait()


def plain_body(w_gate, w_up, router_weight, router_gain):
    scale_gate, scale_up = lax.pmax(
        (jnp.max(jnp.abs(w_gate), axis=1), jnp.max(jnp.abs(w_up), axis=1)), "shard"
    )
    narrow_gate, narrow_up = (
        (w_gate / jnp.expand_dims(scale_gate, 1)).astype(jnp.bfloat16),
        (w_up / jnp.expand_dims(scale_up, 1)).astype(jnp.bfloat16),
    )
    serve_gate, serve_up = (
        lax.all_to_all(narrow_gate, "shard", split_axis=2, concat_axis=1, tiled=True),
        lax.all_to_all(narrow_up, "shard", split_axis=2, concat_axis=1, tiled=True),
    )
    scale_gate = lax.dynamic_slice_in_dim(
        scale_gate, lax.axis_index("shard") * serve_gate.shape[2], serve_gate.shape[2], axis=1
    )
    scale_up = lax.dynamic_slice_in_dim(
        scale_up, lax.axis_index("shard") * serve_up.shape[2], serve_up.shape[2], axis=1
    )
    part_router = (router_weight * router_gain[:, None]).astype(jnp.bfloat16)
    row_router = lax.all_gather(part_router, "shard", axis=0, tiled=True)
    serve_router = lax.all_gather(row_router, "expert", axis=1, tiled=True)
    return (serve_gate, serve_up, scale_gate, scale_up, serve_router)


def body(n, ne, w_gate, w_up, router_weight, router_gain):
    experts, rows, cols = w_gate.shape
    total, h = 2 * experts, n // 2
    fits = (
        n % 2 == 0 and rows % LANES == 0 and cols % LANES == 0 and (cols // n) % 16 == 0
        and total > DIRECT and (total - DIRECT) % h == 0 and (total - DIRECT) % CHUNK == 0
        and total >= SLOTS
    )
    if not fits:
        return plain_body(w_gate, w_up, router_weight, router_gain)
    part, share, local_e = cols // n, (total - DIRECT) // h, router_weight.shape[1]
    dma = pltpu.SemaphoreType.DMA
    anywhere = pl.BlockSpec(memory_space=pl.ANY)
    local = pl.BlockSpec(memory_space=pltpu.VMEM)
    serve, scale, router = pl.pallas_call(
        functools.partial(kernel, n, ne),
        out_shape=(
            pltpu.VMEM((total, part, n * rows), jnp.bfloat16),
            pltpu.VMEM((total, part), jnp.float32),
            pltpu.VMEM((n * rows, ne * local_e), jnp.bfloat16),
        ),
        in_specs=[anywhere, anywhere, local, local],
        out_specs=(local, local, local),
        scratch_shapes=[
            pltpu.VMEM((total, 1, cols), jnp.float32),
            pltpu.VMEM((SLOTS, rows, cols), jnp.float32),
            pltpu.VMEM((total, cols, rows), jnp.bfloat16),
            pltpu.VMEM((total, 1, cols), jnp.float32),
            pltpu.VMEM((n, DIRECT, 1, cols), jnp.float32),
            pltpu.VMEM((h, share, 1, cols), jnp.float32),
            pltpu.VMEM((share, 1, cols), jnp.float32),
            pltpu.VMEM((share, 1, cols), jnp.float32),
            pltpu.VMEM((ne, n, local_e, rows), jnp.bfloat16),
            dma((SLOTS,)),
            dma((n,)),
            dma((n,)),
            dma((2, n)),
            dma((2, n)),
            dma((h,)),
            dma((h,)),
            dma,
            dma,
            dma((h,)),
            dma((h,)),
            dma,
            dma,
            dma((h, 2)),
            dma((h, 2)),
            dma((ne,)),
            dma((ne,)),
        ],
        compiler_params=pltpu.CompilerParams(
            collective_id=0, has_side_effects=True, vmem_limit_bytes=34 * 2**20
        ),
        cost_estimate=pl.CostEstimate(
            flops=4 * experts * rows * cols, bytes_accessed=20 * experts * rows * cols, transcendentals=0
        ),
    )(w_gate, w_up, router_weight.T, router_gain[None, :])
    gate, up, scale_gate, scale_up, router = pl.pallas_call(
        place,
        out_shape=(
            pltpu.HBM((experts, part, n * rows), jnp.bfloat16),
            pltpu.HBM((experts, part, n * rows), jnp.bfloat16),
            pltpu.HBM((experts, part), jnp.float32),
            pltpu.HBM((experts, part), jnp.float32),
            pltpu.HBM((n * rows, ne * local_e), jnp.bfloat16),
        ),
        in_specs=[local] * 3,
        out_specs=(anywhere,) * 5,
        scratch_shapes=[dma((2 * PLACES + 3,))],
        compiler_params=pltpu.CompilerParams(vmem_limit_bytes=2**20),
        cost_estimate=pl.CostEstimate(
            flops=0, bytes_accessed=4 * experts * rows * cols, transcendentals=0
        ),
    )(serve, scale, router)
    return (jnp.swapaxes(gate, 1, 2), jnp.swapaxes(up, 1, 2), scale_gate, scale_up, router)


def solution(mesh):
    return jax.shard_map(
        functools.partial(body, mesh.shape["shard"], mesh.shape["expert"]),
        mesh=mesh,
        in_specs=(
            P("expert", "shard", None),
            P("expert", "shard", None),
            P("shard", "expert"),
            P("shard"),
        ),
        out_specs=(
            P("expert", None, "shard"),
            P("expert", None, "shard"),
            P("expert", "shard"),
            P("expert", "shard"),
            P(),
        ),
        check_vma=False,
    )
```

```python
import functools

import jax
import jax.numpy as jnp
from jax import lax
from jax.experimental import pallas as pl
from jax.experimental.pallas import tpu as pltpu
from jax.sharding import PartitionSpec as P

MESH = pl.DeviceIdType.MESH
SLOTS = 8
LANES = 128
NOW = 2
DIRECT = 8
EARLY = 3
SECOND = 16
SHORT = 8
CHUNK = 2
PLACES = 8


def kernel(
    n, ne,
    gate, up, router, gain,
    serve, late, out_scale, out_router,
    gm, ring, raw, send, lmax, dbuf, ebuf, e_half, e_far, rsbuf, half_max, xbuf, rbuf,
    load_sem, send_sem, recv_sem,
    d_send, d_recv, e_send, e_recv, y_send, y_recv, rs_send, rs_recv, x_send, x_recv, ag_send, ag_recv,
    r0_send, r0_recv, r1_send, r1_recv, r2_send, r2_recv,
):
    me = lax.axis_index("shard")
    my_e = lax.axis_index("expert")
    experts, rows, cols = gate.shape
    part = cols // n
    total = 2 * experts
    lo, hi = total - SECOND, total - SHORT
    h = n // 2
    mine = lax.rem(me, h)
    base = me - mine
    far = (n - h) - base
    share = (total - DIRECT) // h
    peers = range(n - 1)

    def there(l):
        if l < h:
            return far + lax.rem(mine + l, h)
        return base + lax.rem(mine + (l - h + 1), h)

    def back(l):
        if l < h:
            return far + lax.rem(mine + (h - l), h)
        return base + lax.rem(mine + (2 * h - 1 - l), h)

    def near(s):
        return base + lax.rem(mine + s, h)

    def near_back(s):
        return base + lax.rem(mine + (h - s), h)

    def remote(src, dst, ssem, rsem, device):
        return pltpu.make_async_remote_copy(
            src_ref=src, dst_ref=dst, send_sem=ssem, recv_sem=rsem,
            device_id=device, device_id_type=MESH,
        )

    def load(array, index, slot):
        return pltpu.make_async_copy(array.at[index], ring.at[slot], load_sem.at[slot])

    again = EARLY - NOW
    loads = 2 * total - NOW

    def item_of(k):
        early = jnp.where(k < DIRECT, k, k - DIRECT + NOW)
        late = jnp.where(k < total + again, k - again, k - total + NOW)
        return jnp.where(k < DIRECT + again, early, late)

    def fetch(k):
        slot = lax.rem(k, SLOTS)
        item = item_of(k)

        @pl.when((k < loads) & (item < experts))
        def _():
            load(gate, item, slot).start()

        @pl.when((k < loads) & (item >= experts))
        def _():
            load(up, item - experts, slot).start()

    for k in range(SLOTS):
        load((gate, up)[k // experts], k % experts, k).start()

    barrier = pltpu.get_barrier_semaphore()
    for l in peers:
        pl.semaphore_signal(barrier, inc=1, device_id={"shard": there(l)}, device_id_type=MESH)
    for r in range(1, ne):
        pl.semaphore_signal(
            barrier, inc=1, device_id={"expert": lax.rem(my_e + r, ne)}, device_id_type=MESH
        )

    def direct(l, slot):
        return remote(
            lmax.at[pl.ds(0, NOW)], dbuf.at[slot], d_send.at[l], d_recv.at[l], {"shard": there(l)}
        )

    soon = pl.ds(NOW, DIRECT - NOW)

    def soon_near(s):
        return remote(lmax.at[soon], ebuf.at[s], e_send.at[s], e_recv.at[s], {"shard": near(s)})

    def soon_far():
        return remote(e_half, e_far, y_send, y_recv, {"shard": far + mine})

    def spread(s, slot):
        return remote(
            lmax.at[pl.ds(DIRECT + lax.rem(mine + s, h) * share, share)], rsbuf.at[s],
            rs_send.at[s], rs_recv.at[s], {"shard": near(s)},
        )

    def swap():
        return remote(half_max, xbuf, x_send, x_recv, {"shard": far + mine})

    def collect(s, slot):
        block = pl.ds(DIRECT + slot * share, share)
        return remote(gm.at[block], gm.at[block], ag_send.at[s], ag_recv.at[s], {"shard": near(s)})

    def router_swap(slot):
        return remote(
            rbuf.at[my_e, me], rbuf.at[my_e, slot], r0_send, r0_recv, {"shard": far + mine}
        )

    def router_row(s, j, slot):
        return remote(
            rbuf.at[my_e, slot], rbuf.at[my_e, slot],
            r1_send.at[s, j], r1_recv.at[s, j], {"shard": near(s)},
        )

    def router_col(r, slot):
        return remote(
            rbuf.at[slot], rbuf.at[slot], r2_send.at[r], r2_recv.at[r],
            {"expert": lax.rem(my_e + r, ne)},
        )

    def column(slot):
        return pl.ds(pl.multiple_of(slot * rows, LANES), rows)

    def peer_rows(slot):
        return pl.ds(pl.multiple_of(slot * part, 16), part)

    def piece(l, slot, first, count, tail=False):
        source = late.at[pl.ds(first - lo, count)] if tail else send.at[pl.ds(first, count)]
        return remote(
            source.at[:, peer_rows(there(l))],
            serve.at[pl.ds(first, count), :, column(slot)],
            send_sem.at[l], recv_sem.at[l], {"shard": there(l)},
        )

    def largest_of(slot, item):
        load(gate, 0, slot).wait()
        lmax[item] = jnp.max(jnp.abs(ring[slot]), axis=0, keepdims=True)

    def maxima(k, item):
        slot = lax.rem(k, SLOTS)
        largest_of(slot, item)
        fetch(k + SLOTS)

    def turn(k):
        for j in range(0, cols, LANES):
            raw[k, j:j + LANES, :] = ring[k, :, j:j + LANES].T
        fetch(k + SLOTS)

    def quotient(k, item, tail=False):
        slot = lax.rem(k, SLOTS)
        load(gate, 0, slot).wait()
        inverse = 1.0 / gm[item]
        for j in range(0, cols, LANES):
            block = ring[slot, :, j:j + LANES] * inverse[:, j:j + LANES]
            if tail:
                late[item - lo, j:j + LANES, :] = block.T.astype(jnp.bfloat16)
            else:
                send[item, j:j + LANES, :] = block.T.astype(jnp.bfloat16)
        fetch(k + SLOTS)
        if not tail:
            keep(item)

    def keep(item):
        serve[item, :, column(me)] = send[item, peer_rows(me), :]

    def first_quotient(item):
        inverse = jnp.broadcast_to(1.0 / gm[item], (8, cols))
        for j in range(0, cols, LANES):
            factor = inverse[:, j:j + LANES].T[:, 0:1]
            send[item, j:j + LANES, :] = (raw[item, j:j + LANES, :] * factor).astype(jnp.bfloat16)
        keep(item)
        ship(item, 1)

    def whole_piece(l, slot, count):
        spot = serve.at[pl.ds(0, count), :, column(slot)]
        return remote(spot, spot, send_sem.at[l], recv_sem.at[l], {"shard": there(l)})

    def ship(first, count, tail=False):
        for l in sorted(peers, key=lambda l: (l % h, l // h)):
            piece(l, me, first, count, tail).start()

    def settle_now():
        largest = lmax[pl.ds(0, NOW)]
        for l in peers:
            direct(l, back(l)).wait_recv()
            largest = jnp.maximum(largest, dbuf[back(l)])
        gm[pl.ds(0, NOW)] = largest

    def settle_half():
        largest = lmax[soon]
        for s in range(1, h):
            soon_near(s).wait_recv()
            largest = jnp.maximum(largest, ebuf[s])
        e_half[...] = largest
        soon_far().start()

    def settle_soon():
        soon_far().wait_recv()
        gm[soon] = jnp.maximum(e_half[...], e_far[...])

    def maxima_span(first, last, shift):
        @pl.loop(first, last)
        def _(item):
            maxima(item + shift, item)

    def quotient_span(first, last, shift):
        @pl.loop(first, last)
        def _(item):
            quotient(item + shift, item)
            ship(item, 1)

    for k in range(NOW):
        largest_of(k, k)
    rbuf[my_e, me] = (router[...] * gain[...]).astype(jnp.bfloat16)
    pl.semaphore_wait(barrier, n + ne - 2)
    for l in peers:
        direct(l, me).start()
    router_swap(me).start()
    for k in range(NOW):
        turn(k)
    maxima_span(NOW, DIRECT, 0)
    for s in range(1, h):
        soon_near(s).start()
    settle_now()
    first_quotient(0)
    settle_half()
    for k in range(1, NOW):
        first_quotient(k)
    settle_soon()
    quotient_span(NOW, EARLY, DIRECT - NOW)
    maxima_span(DIRECT, total, again)

    for s in range(1, h):
        spread(s, mine).start()
    quotient_span(EARLY, EARLY + 1, loads - total)
    largest = lmax[pl.ds(DIRECT + mine * share, share)]
    for s in range(1, h):
        spread(s, mine).wait_recv()
        largest = jnp.maximum(largest, rsbuf[s])
    half_max[...] = largest
    router_swap(far + mine).wait_recv()
    swap().start()
    for s in range(1, h):
        router_row(s, 0, me).start()
        router_row(s, 1, far + mine).start()
    quotient_span(EARLY + 1, EARLY + 2, loads - total)
    swap().wait_recv()
    gm[pl.ds(DIRECT + mine * share, share)] = jnp.maximum(half_max[...], xbuf[...])
    quotient_span(EARLY + 2, EARLY + 3, loads - total)
    for s in range(1, h):
        collect(s, mine).start()
    quotient_span(EARLY + 3, DIRECT, loads - total)
    for s in range(1, h):
        collect(s, lax.rem(mine + (h - s), h)).wait_recv()

    @pl.loop(0, (lo - DIRECT) // CHUNK)
    def _(c):
        first = DIRECT + c * CHUNK

        @pl.loop(0, CHUNK)
        def _(i):
            quotient(loads - total + first + i, first + i)

        @pl.when(c > 0)
        def _():
            ship(first - CHUNK, CHUNK)

    longer = lax.rem(my_e, 2) == 1

    @pl.loop(0, SECOND // CHUNK)
    def _(c):
        first = lo + c * CHUNK

        @pl.loop(0, CHUNK)
        def _(i):
            quotient(loads - total + first + i, first + i, True)

        @pl.when(c == 0)
        def _():
            ship(lo - CHUNK, CHUNK)

        @pl.when((c > 0) & (first <= hi) & longer)
        def _():
            ship(first - CHUNK, CHUNK, True)

    @pl.when(longer)
    def _():
        serve[pl.ds(lo, hi - lo), :, column(me)] = late[pl.ds(0, hi - lo), peer_rows(me), :]

    for s in range(1, h):
        router_row(s, 0, near_back(s)).wait_recv()
        router_row(s, 1, far + lax.rem(mine + (h - s), h)).wait_recv()
    for r in range(1, ne):
        router_col(r, my_e).start()
    whole = gm[...].reshape(total, cols)
    for s in range(n):
        @pl.when(me == s)
        def _():
            out_scale[...] = whole[:, s * part:(s + 1) * part]
    for r in range(1, ne):
        router_col(r, lax.rem(my_e + (ne - r), ne)).wait_recv()
    for s in range(n):
        block = rbuf[:, s].astype(jnp.float32).reshape(ne * rbuf.shape[2], rows)
        out_router[s * rows:(s + 1) * rows, :] = block.T.astype(jnp.bfloat16)

    for l in peers:
        direct(l, me).wait_send()
    soon_far().wait_send()
    for s in range(1, h):
        soon_near(s).wait_send()
        spread(s, mine).wait_send()
        collect(s, mine).wait_send()
        router_row(s, 0, me).wait_send()
        router_row(s, 1, far + mine).wait_send()
    swap().wait_send()
    router_swap(me).wait_send()
    for r in range(1, ne):
        router_col(r, my_e).wait_send()
    @pl.when(longer)
    def _():
        for l in peers:
            whole_piece(l, me, hi).wait_send()
        for l in peers:
            whole_piece(l, back(l), hi).wait_recv()

    @pl.when(jnp.logical_not(longer))
    def _():
        for l in peers:
            whole_piece(l, me, lo).wait_send()
        for l in peers:
            whole_piece(l, back(l), lo).wait_recv()


def second(n, late, _, serve, send_sem, recv_sem):
    me = lax.axis_index("shard")
    my_e = lax.axis_index("expert")
    rows = late.shape[2]
    part = late.shape[1] // n
    h = n // 2
    mine = lax.rem(me, h)
    base = me - mine
    far = (n - h) - base
    peers = range(n - 1)

    def there(l):
        if l < h:
            return far + lax.rem(mine + l, h)
        return base + lax.rem(mine + (l - h + 1), h)

    def back(l):
        if l < h:
            return far + lax.rem(mine + (h - l), h)
        return base + lax.rem(mine + (2 * h - 1 - l), h)

    def column(slot):
        return pl.ds(pl.multiple_of(slot * rows, LANES), rows)

    def peer_rows(slot):
        return pl.ds(pl.multiple_of(slot * part, 16), part)

    def piece(l, slot, first, count):
        return pltpu.make_async_remote_copy(
            src_ref=late.at[pl.ds(first, count), peer_rows(there(l))],
            dst_ref=serve.at[pl.ds(first, count), :, column(slot)],
            send_sem=send_sem.at[l], recv_sem=recv_sem.at[l],
            device_id={"shard": there(l)}, device_id_type=MESH,
        )

    barrier = pltpu.get_barrier_semaphore()
    for l in peers:
        pl.semaphore_signal(barrier, inc=1, device_id={"shard": there(l)}, device_id_type=MESH)
    serve[:, :, column(me)] = late[:, peer_rows(me), :]
    pl.semaphore_wait(barrier, n - 1)

    def exchange(start):
        @pl.loop(0, (SECOND - start) // CHUNK)
        def _(c):
            for l in sorted(peers, key=lambda l: (l % h, l // h)):
                piece(l, me, start + c * CHUNK, CHUNK).start()

        for l in peers:
            piece(l, me, start, SECOND - start).wait_send()
        for l in peers:
            piece(l, back(l), start, SECOND - start).wait_recv()

    @pl.when(lax.rem(my_e, 2) == 0)
    def _():
        exchange(0)

    @pl.when(lax.rem(my_e, 2) == 1)
    def _():
        exchange(SECOND - SHORT)


def run_all(moves, sems):
    copies = [pltpu.make_async_copy(a, b, sems.at[i]) for i, (a, b) in enumerate(moves)]
    for copy in copies:
        copy.start()
    for copy in copies:
        copy.wait()


def place(lo, serve, scale, router, out_gate, out_up, out_sg, out_su, out_router, token, sems):
    experts = out_gate.shape[0]
    step = experts // PLACES
    moves = [
        (serve.at[pl.ds(i * step, step)], out_gate.at[pl.ds(i * step, step)])
        for i in range(PLACES)
    ]
    rest = lo - experts
    cuts = [rest * i // PLACES for i in range(PLACES + 1)]
    moves += [
        (serve.at[pl.ds(experts + a, b - a)], out_up.at[pl.ds(a, b - a)])
        for a, b in zip(cuts, cuts[1:])
    ]
    moves += [
        (router, out_router),
        (scale.at[pl.ds(0, experts)], out_sg),
        (scale.at[pl.ds(experts, experts)], out_su),
        (scale.at[pl.ds(0, 8)], token),
    ]
    run_all(moves, sems)


def place_second(lo, serve, tail, _, out_up, sems):
    experts = out_up.shape[0]
    spot = lo - experts
    gap = SECOND - SHORT

    def cut(source, at, to, count):
        half = count // 2
        return [
            (source.at[pl.ds(at, half)], out_up.at[pl.ds(to, half)]),
            (source.at[pl.ds(at + half, count - half)], out_up.at[pl.ds(to + half, count - half)]),
        ]

    longer = lax.rem(lax.axis_index("expert"), 2) == 1

    @pl.when(longer)
    def _():
        run_all(cut(serve, lo, spot, gap) + cut(tail, gap, spot + gap, SHORT), sems)

    @pl.when(jnp.logical_not(longer))
    def _():
        run_all(cut(tail, 0, spot, gap) + cut(tail, gap, spot + gap, SHORT), sems)


def plain_body(w_gate, w_up, router_weight, router_gain):
    scale_gate, scale_up = lax.pmax(
        (jnp.max(jnp.abs(w_gate), axis=1), jnp.max(jnp.abs(w_up), axis=1)), "shard"
    )
    narrow_gate, narrow_up = (
        (w_gate / jnp.expand_dims(scale_gate, 1)).astype(jnp.bfloat16),
        (w_up / jnp.expand_dims(scale_up, 1)).astype(jnp.bfloat16),
    )
    serve_gate, serve_up = (
        lax.all_to_all(narrow_gate, "shard", split_axis=2, concat_axis=1, tiled=True),
        lax.all_to_all(narrow_up, "shard", split_axis=2, concat_axis=1, tiled=True),
    )
    scale_gate = lax.dynamic_slice_in_dim(
        scale_gate, lax.axis_index("shard") * serve_gate.shape[2], serve_gate.shape[2], axis=1
    )
    scale_up = lax.dynamic_slice_in_dim(
        scale_up, lax.axis_index("shard") * serve_up.shape[2], serve_up.shape[2], axis=1
    )
    part_router = (router_weight * router_gain[:, None]).astype(jnp.bfloat16)
    row_router = lax.all_gather(part_router, "shard", axis=0, tiled=True)
    serve_router = lax.all_gather(row_router, "expert", axis=1, tiled=True)
    return (serve_gate, serve_up, scale_gate, scale_up, serve_router)


def body(n, ne, w_gate, w_up, router_weight, router_gain):
    experts, rows, cols = w_gate.shape
    total, h = 2 * experts, n // 2
    fits = (
        n % 2 == 0 and rows % LANES == 0 and cols % LANES == 0 and (cols // n) % 16 == 0
        and total > DIRECT and (total - DIRECT) % h == 0 and (total - DIRECT) % CHUNK == 0
        and total >= SLOTS and total - SECOND >= max(experts + PLACES, DIRECT + CHUNK)
        and (total - SECOND - DIRECT) % CHUNK == 0 and experts % PLACES == 0
    )
    if not fits:
        return plain_body(w_gate, w_up, router_weight, router_gain)
    part, share, local_e = cols // n, (total - DIRECT) // h, router_weight.shape[1]
    lo, hi = total - SECOND, total - SHORT
    dma = pltpu.SemaphoreType.DMA
    anywhere = pl.BlockSpec(memory_space=pl.ANY)
    local = pl.BlockSpec(memory_space=pltpu.VMEM)
    serve, late, scale, router = pl.pallas_call(
        functools.partial(kernel, n, ne),
        out_shape=(
            pltpu.VMEM((hi, part, n * rows), jnp.bfloat16),
            pltpu.VMEM((SECOND, cols, rows), jnp.bfloat16),
            pltpu.VMEM((total, part), jnp.float32),
            pltpu.VMEM((n * rows, ne * local_e), jnp.bfloat16),
        ),
        in_specs=[anywhere, anywhere, local, local],
        out_specs=(local, local, local, local),
        scratch_shapes=[
            pltpu.VMEM((total, 1, cols), jnp.float32),
            pltpu.VMEM((SLOTS, rows, cols), jnp.float32),
            pltpu.VMEM((NOW, cols, rows), jnp.float32),
            pltpu.VMEM((lo, cols, rows), jnp.bfloat16),
            pltpu.VMEM((total, 1, cols), jnp.float32),
            pltpu.VMEM((n, NOW, 1, cols), jnp.float32),
            pltpu.VMEM((h, DIRECT - NOW, 1, cols), jnp.float32),
            pltpu.VMEM((DIRECT - NOW, 1, cols), jnp.float32),
            pltpu.VMEM((DIRECT - NOW, 1, cols), jnp.float32),
            pltpu.VMEM((h, share, 1, cols), jnp.float32),
            pltpu.VMEM((share, 1, cols), jnp.float32),
            pltpu.VMEM((share, 1, cols), jnp.float32),
            pltpu.VMEM((ne, n, local_e, rows), jnp.bfloat16),
            dma((SLOTS,)),
            dma((n,)),
            dma((n,)),
            dma((n,)),
            dma((n,)),
            dma((h,)),
            dma((h,)),
            dma,
            dma,
            dma((h,)),
            dma((h,)),
            dma,
            dma,
            dma((h,)),
            dma((h,)),
            dma,
            dma,
            dma((h, 2)),
            dma((h, 2)),
            dma((ne,)),
            dma((ne,)),
        ],
        compiler_params=pltpu.CompilerParams(
            collective_id=0, has_side_effects=True, vmem_limit_bytes=30 * 2**20
        ),
        cost_estimate=pl.CostEstimate(
            flops=4 * experts * rows * cols, bytes_accessed=20 * experts * rows * cols, transcendentals=0
        ),
    )(w_gate, w_up, router_weight.T, router_gain[None, :])
    gate, up, scale_gate, scale_up, router, token = pl.pallas_call(
        functools.partial(place, lo),
        out_shape=(
            pltpu.HBM((experts, part, n * rows), jnp.bfloat16),
            pltpu.HBM((experts, part, n * rows), jnp.bfloat16),
            pltpu.HBM((experts, part), jnp.float32),
            pltpu.HBM((experts, part), jnp.float32),
            pltpu.HBM((n * rows, ne * local_e), jnp.bfloat16),
            pltpu.HBM((8, part), jnp.float32),
        ),
        in_specs=[local] * 3,
        out_specs=(anywhere,) * 6,
        scratch_shapes=[dma((2 * PLACES + 4,))],
        compiler_params=pltpu.CompilerParams(vmem_limit_bytes=2**20),
        cost_estimate=pl.CostEstimate(
            flops=0, bytes_accessed=4 * experts * rows * cols, transcendentals=0
        ),
    )(serve, scale, router)
    tail = pl.pallas_call(
        functools.partial(second, n),
        out_shape=pltpu.VMEM((SECOND, part, n * rows), jnp.bfloat16),
        in_specs=[local, anywhere],
        out_specs=local,
        scratch_shapes=[dma((n,)), dma((n,))],
        compiler_params=pltpu.CompilerParams(
            collective_id=1, has_side_effects=True, vmem_limit_bytes=2**20
        ),
        cost_estimate=pl.CostEstimate(
            flops=0, bytes_accessed=SECOND * rows * cols, transcendentals=0
        ),
    )(late, token)
    up = pl.pallas_call(
        functools.partial(place_second, lo),
        out_shape=pltpu.HBM((experts, part, n * rows), jnp.bfloat16),
        in_specs=[local, local, anywhere],
        out_specs=anywhere,
        input_output_aliases={2: 0},
        scratch_shapes=[dma((4,))],
        compiler_params=pltpu.CompilerParams(vmem_limit_bytes=2**20),
        cost_estimate=pl.CostEstimate(
            flops=0, bytes_accessed=4 * SECOND * rows * cols, transcendentals=0
        ),
    )(serve, tail, up)
    return (jnp.swapaxes(gate, 1, 2), jnp.swapaxes(up, 1, 2), scale_gate, scale_up, router)


def solution(mesh):
    return jax.shard_map(
        functools.partial(body, mesh.shape["shard"], mesh.shape["expert"]),
        mesh=mesh,
        in_specs=(
            P("expert", "shard", None),
            P("expert", "shard", None),
            P("shard", "expert"),
            P("shard"),
        ),
        out_specs=(
            P("expert", None, "shard"),
            P("expert", None, "shard"),
            P("expert", "shard"),
            P("expert", "shard"),
            P(),
        ),
        check_vma=False,
    )
```

```python
import functools

import jax
import jax.numpy as jnp
from jax import lax
from jax.experimental import pallas as pl
from jax.experimental.pallas import tpu as pltpu
from jax.sharding import PartitionSpec as P

MESH = pl.DeviceIdType.MESH
SLOTS = 8
LANES = 128
NOW = 2
DIRECT = 8
EARLY = 3
SECOND = 10
SHORT = 2
CHUNK = 2
PLACES = 8


def kernel(
    n, ne,
    gate, up, router, gain,
    serve, late, out_scale, out_router,
    gm, ring, raw, send, lmax, dbuf, ebuf, e_half, e_far, rsbuf, half_max, xbuf, rbuf,
    load_sem, send_sem, recv_sem,
    d_send, d_recv, e_send, e_recv, y_send, y_recv, rs_send, rs_recv, x_send, x_recv, ag_send, ag_recv,
    r0_send, r0_recv, r1_send, r1_recv, r2_send, r2_recv,
):
    me = lax.axis_index("shard")
    my_e = lax.axis_index("expert")
    experts, rows, cols = gate.shape
    part = cols // n
    total = 2 * experts
    lo, hi = total - SECOND, total - SHORT
    h = n // 2
    mine = lax.rem(me, h)
    base = me - mine
    far = (n - h) - base
    share = (total - DIRECT) // h
    peers = range(n - 1)

    def there(l):
        if l < h:
            return far + lax.rem(mine + l, h)
        return base + lax.rem(mine + (l - h + 1), h)

    def back(l):
        if l < h:
            return far + lax.rem(mine + (h - l), h)
        return base + lax.rem(mine + (2 * h - 1 - l), h)

    def near(s):
        return base + lax.rem(mine + s, h)

    def near_back(s):
        return base + lax.rem(mine + (h - s), h)

    def remote(src, dst, ssem, rsem, device):
        return pltpu.make_async_remote_copy(
            src_ref=src, dst_ref=dst, send_sem=ssem, recv_sem=rsem,
            device_id=device, device_id_type=MESH,
        )

    def load(array, index, slot):
        return pltpu.make_async_copy(array.at[index], ring.at[slot], load_sem.at[slot])

    again = EARLY - NOW
    loads = 2 * total - NOW

    def item_of(k):
        early = jnp.where(k < DIRECT, k, k - DIRECT + NOW)
        late = jnp.where(k < total + again, k - again, k - total + NOW)
        return jnp.where(k < DIRECT + again, early, late)

    def fetch(k):
        slot = lax.rem(k, SLOTS)
        item = item_of(k)

        @pl.when((k < loads) & (item < experts))
        def _():
            load(gate, item, slot).start()

        @pl.when((k < loads) & (item >= experts))
        def _():
            load(up, item - experts, slot).start()

    for k in range(SLOTS):
        load((gate, up)[k // experts], k % experts, k).start()

    barrier = pltpu.get_barrier_semaphore()
    for l in peers:
        pl.semaphore_signal(barrier, inc=1, device_id={"shard": there(l)}, device_id_type=MESH)
    for r in range(1, ne):
        pl.semaphore_signal(
            barrier, inc=1, device_id={"expert": lax.rem(my_e + r, ne)}, device_id_type=MESH
        )

    def direct(l, slot):
        return remote(
            lmax.at[pl.ds(0, NOW)], dbuf.at[slot], d_send.at[l], d_recv.at[l], {"shard": there(l)}
        )

    soon = pl.ds(NOW, DIRECT - NOW)

    def soon_near(s):
        return remote(lmax.at[soon], ebuf.at[s], e_send.at[s], e_recv.at[s], {"shard": near(s)})

    def soon_far():
        return remote(e_half, e_far, y_send, y_recv, {"shard": far + mine})

    def spread(s, slot):
        return remote(
            lmax.at[pl.ds(DIRECT + lax.rem(mine + s, h) * share, share)], rsbuf.at[s],
            rs_send.at[s], rs_recv.at[s], {"shard": near(s)},
        )

    def swap():
        return remote(half_max, xbuf, x_send, x_recv, {"shard": far + mine})

    def collect(s, slot):
        block = pl.ds(DIRECT + slot * share, share)
        return remote(gm.at[block], gm.at[block], ag_send.at[s], ag_recv.at[s], {"shard": near(s)})

    def router_swap(slot):
        return remote(
            rbuf.at[my_e, me], rbuf.at[my_e, slot], r0_send, r0_recv, {"shard": far + mine}
        )

    def router_row(s, j, slot):
        return remote(
            rbuf.at[my_e, slot], rbuf.at[my_e, slot],
            r1_send.at[s, j], r1_recv.at[s, j], {"shard": near(s)},
        )

    def router_col(r, slot):
        return remote(
            rbuf.at[slot], rbuf.at[slot], r2_send.at[r], r2_recv.at[r],
            {"expert": lax.rem(my_e + r, ne)},
        )

    def column(slot):
        return pl.ds(pl.multiple_of(slot * rows, LANES), rows)

    def peer_rows(slot):
        return pl.ds(pl.multiple_of(slot * part, 16), part)

    def piece(l, slot, first, count, tail=False):
        source = late.at[pl.ds(first - lo, count)] if tail else send.at[pl.ds(first, count)]
        return remote(
            source.at[:, peer_rows(there(l))],
            serve.at[pl.ds(first, count), :, column(slot)],
            send_sem.at[l], recv_sem.at[l], {"shard": there(l)},
        )

    def largest_of(slot, item):
        load(gate, 0, slot).wait()
        lmax[item] = jnp.max(jnp.abs(ring[slot]), axis=0, keepdims=True)

    def maxima(k, item):
        slot = lax.rem(k, SLOTS)
        largest_of(slot, item)
        fetch(k + SLOTS)

    def turn(k):
        for j in range(0, cols, LANES):
            raw[k, j:j + LANES, :] = ring[k, :, j:j + LANES].T
        fetch(k + SLOTS)

    def quotient(k, item, tail=False):
        slot = lax.rem(k, SLOTS)
        load(gate, 0, slot).wait()
        inverse = 1.0 / gm[item]
        for j in range(0, cols, LANES):
            block = ring[slot, :, j:j + LANES] * inverse[:, j:j + LANES]
            if tail:
                late[item - lo, j:j + LANES, :] = block.T.astype(jnp.bfloat16)
            else:
                send[item, j:j + LANES, :] = block.T.astype(jnp.bfloat16)
        fetch(k + SLOTS)
        if not tail:
            keep(item)

    def keep(item):
        serve[item, :, column(me)] = send[item, peer_rows(me), :]

    def first_quotient(item):
        inverse = jnp.broadcast_to(1.0 / gm[item], (8, cols))
        for j in range(0, cols, LANES):
            factor = inverse[:, j:j + LANES].T[:, 0:1]
            send[item, j:j + LANES, :] = (raw[item, j:j + LANES, :] * factor).astype(jnp.bfloat16)
        keep(item)
        ship(item, 1)

    def whole_piece(l, slot, count):
        spot = serve.at[pl.ds(0, count), :, column(slot)]
        return remote(spot, spot, send_sem.at[l], recv_sem.at[l], {"shard": there(l)})

    def ship(first, count, tail=False):
        for l in sorted(peers, key=lambda l: (l % h, l // h)):
            piece(l, me, first, count, tail).start()

    def settle_now():
        largest = lmax[pl.ds(0, NOW)]
        for l in peers:
            direct(l, back(l)).wait_recv()
            largest = jnp.maximum(largest, dbuf[back(l)])
        gm[pl.ds(0, NOW)] = largest

    def settle_half():
        largest = lmax[soon]
        for s in range(1, h):
            soon_near(s).wait_recv()
            largest = jnp.maximum(largest, ebuf[s])
        e_half[...] = largest
        soon_far().start()

    def settle_soon():
        soon_far().wait_recv()
        gm[soon] = jnp.maximum(e_half[...], e_far[...])

    def maxima_span(first, last, shift):
        @pl.loop(first, last)
        def _(item):
            maxima(item + shift, item)

    def quotient_span(first, last, shift):
        @pl.loop(first, last)
        def _(item):
            quotient(item + shift, item)
            ship(item, 1)

    for k in range(NOW):
        largest_of(k, k)
    rbuf[my_e, me] = (router[...] * gain[...]).astype(jnp.bfloat16)
    pl.semaphore_wait(barrier, n + ne - 2)
    for l in peers:
        direct(l, me).start()
    router_swap(me).start()
    for k in range(NOW):
        turn(k)
    maxima_span(NOW, DIRECT, 0)
    for s in range(1, h):
        soon_near(s).start()
    settle_now()
    first_quotient(0)
    settle_half()
    for k in range(1, NOW):
        first_quotient(k)
    settle_soon()
    quotient_span(NOW, EARLY, DIRECT - NOW)
    maxima_span(DIRECT, total, again)

    for s in range(1, h):
        spread(s, mine).start()
    quotient_span(EARLY, EARLY + 1, loads - total)
    largest = lmax[pl.ds(DIRECT + mine * share, share)]
    for s in range(1, h):
        spread(s, mine).wait_recv()
        largest = jnp.maximum(largest, rsbuf[s])
    half_max[...] = largest
    router_swap(far + mine).wait_recv()
    swap().start()
    for s in range(1, h):
        router_row(s, 0, me).start()
        router_row(s, 1, far + mine).start()
    quotient_span(EARLY + 1, EARLY + 2, loads - total)
    swap().wait_recv()
    gm[pl.ds(DIRECT + mine * share, share)] = jnp.maximum(half_max[...], xbuf[...])
    quotient_span(EARLY + 2, EARLY + 3, loads - total)
    for s in range(1, h):
        collect(s, mine).start()
    quotient_span(EARLY + 3, DIRECT, loads - total)
    for s in range(1, h):
        collect(s, lax.rem(mine + (h - s), h)).wait_recv()

    @pl.loop(0, (lo - DIRECT) // CHUNK)
    def _(c):
        first = DIRECT + c * CHUNK

        @pl.loop(0, CHUNK)
        def _(i):
            quotient(loads - total + first + i, first + i)

        @pl.when(c > 0)
        def _():
            ship(first - CHUNK, CHUNK)

    longer = lax.rem(my_e, 2) == 1

    @pl.loop(0, SECOND // CHUNK)
    def _(c):
        first = lo + c * CHUNK

        @pl.loop(0, CHUNK)
        def _(i):
            quotient(loads - total + first + i, first + i, True)

        @pl.when(c == 0)
        def _():
            ship(lo - CHUNK, CHUNK)

        @pl.when((c > 0) & (first <= hi) & longer)
        def _():
            ship(first - CHUNK, CHUNK, True)

    @pl.when(longer)
    def _():
        serve[pl.ds(lo, hi - lo), :, column(me)] = late[pl.ds(0, hi - lo), peer_rows(me), :]

    for s in range(1, h):
        router_row(s, 0, near_back(s)).wait_recv()
        router_row(s, 1, far + lax.rem(mine + (h - s), h)).wait_recv()
    for r in range(1, ne):
        router_col(r, my_e).start()
    whole = gm[...].reshape(total, cols)
    for s in range(n):
        @pl.when(me == s)
        def _():
            out_scale[...] = whole[:, s * part:(s + 1) * part]
    for r in range(1, ne):
        router_col(r, lax.rem(my_e + (ne - r), ne)).wait_recv()
    for s in range(n):
        block = rbuf[:, s].astype(jnp.float32).reshape(ne * rbuf.shape[2], rows)
        out_router[s * rows:(s + 1) * rows, :] = block.T.astype(jnp.bfloat16)

    for l in peers:
        direct(l, me).wait_send()
    soon_far().wait_send()
    for s in range(1, h):
        soon_near(s).wait_send()
        spread(s, mine).wait_send()
        collect(s, mine).wait_send()
        router_row(s, 0, me).wait_send()
        router_row(s, 1, far + mine).wait_send()
    swap().wait_send()
    router_swap(me).wait_send()
    for r in range(1, ne):
        router_col(r, my_e).wait_send()
    @pl.when(longer)
    def _():
        for l in peers:
            whole_piece(l, me, hi).wait_send()
        for l in peers:
            whole_piece(l, back(l), hi).wait_recv()

    @pl.when(jnp.logical_not(longer))
    def _():
        for l in peers:
            whole_piece(l, me, lo).wait_send()
        for l in peers:
            whole_piece(l, back(l), lo).wait_recv()


def second(n, late, _, serve, send_sem, recv_sem):
    me = lax.axis_index("shard")
    my_e = lax.axis_index("expert")
    rows = late.shape[2]
    part = late.shape[1] // n
    h = n // 2
    mine = lax.rem(me, h)
    base = me - mine
    far = (n - h) - base
    peers = range(n - 1)

    def there(l):
        if l < h:
            return far + lax.rem(mine + l, h)
        return base + lax.rem(mine + (l - h + 1), h)

    def back(l):
        if l < h:
            return far + lax.rem(mine + (h - l), h)
        return base + lax.rem(mine + (2 * h - 1 - l), h)

    def column(slot):
        return pl.ds(pl.multiple_of(slot * rows, LANES), rows)

    def peer_rows(slot):
        return pl.ds(pl.multiple_of(slot * part, 16), part)

    def piece(l, slot, first, count):
        return pltpu.make_async_remote_copy(
            src_ref=late.at[pl.ds(first, count), peer_rows(there(l))],
            dst_ref=serve.at[pl.ds(first, count), :, column(slot)],
            send_sem=send_sem.at[l], recv_sem=recv_sem.at[l],
            device_id={"shard": there(l)}, device_id_type=MESH,
        )

    barrier = pltpu.get_barrier_semaphore()
    for l in peers:
        pl.semaphore_signal(barrier, inc=1, device_id={"shard": there(l)}, device_id_type=MESH)
    serve[:, :, column(me)] = late[:, peer_rows(me), :]
    pl.semaphore_wait(barrier, n - 1)

    def exchange(start):
        @pl.loop(start, SECOND)
        def _(c):
            for l in sorted(peers, key=lambda l: (l % h, l // h)):
                piece(l, me, c, 1).start()

        for l in peers:
            piece(l, me, start, SECOND - start).wait_send()
        for l in peers:
            piece(l, back(l), start, SECOND - start).wait_recv()

    @pl.when(lax.rem(my_e, 2) == 0)
    def _():
        exchange(0)

    @pl.when(lax.rem(my_e, 2) == 1)
    def _():
        exchange(SECOND - SHORT)


def run_all(moves, sems):
    copies = [pltpu.make_async_copy(a, b, sems.at[i]) for i, (a, b) in enumerate(moves)]
    for copy in copies:
        copy.start()
    for copy in copies:
        copy.wait()


def place(lo, serve, scale, router, out_gate, out_up, out_sg, out_su, out_router, token, sems):
    experts = out_gate.shape[0]
    step = experts // PLACES
    moves = [
        (serve.at[pl.ds(i * step, step)], out_gate.at[pl.ds(i * step, step)])
        for i in range(PLACES)
    ]
    rest = lo - experts
    cuts = [rest * i // PLACES for i in range(PLACES + 1)]
    moves += [
        (serve.at[pl.ds(experts + a, b - a)], out_up.at[pl.ds(a, b - a)])
        for a, b in zip(cuts, cuts[1:])
    ]
    moves += [
        (router, out_router),
        (scale.at[pl.ds(0, experts)], out_sg),
        (scale.at[pl.ds(experts, experts)], out_su),
        (scale.at[pl.ds(0, 8)], token),
    ]
    run_all(moves, sems)


def place_second(lo, serve, tail, _, out_up, sems):
    experts = out_up.shape[0]
    spot = lo - experts
    gap = SECOND - SHORT

    def cut(source, at, to, count):
        half = count // 2
        return [
            (source.at[pl.ds(at, half)], out_up.at[pl.ds(to, half)]),
            (source.at[pl.ds(at + half, count - half)], out_up.at[pl.ds(to + half, count - half)]),
        ]

    longer = lax.rem(lax.axis_index("expert"), 2) == 1

    @pl.when(longer)
    def _():
        run_all(cut(serve, lo, spot, gap) + cut(tail, gap, spot + gap, SHORT), sems)

    @pl.when(jnp.logical_not(longer))
    def _():
        run_all(cut(tail, 0, spot, gap) + cut(tail, gap, spot + gap, SHORT), sems)


def plain_body(w_gate, w_up, router_weight, router_gain):
    scale_gate, scale_up = lax.pmax(
        (jnp.max(jnp.abs(w_gate), axis=1), jnp.max(jnp.abs(w_up), axis=1)), "shard"
    )
    narrow_gate, narrow_up = (
        (w_gate / jnp.expand_dims(scale_gate, 1)).astype(jnp.bfloat16),
        (w_up / jnp.expand_dims(scale_up, 1)).astype(jnp.bfloat16),
    )
    serve_gate, serve_up = (
        lax.all_to_all(narrow_gate, "shard", split_axis=2, concat_axis=1, tiled=True),
        lax.all_to_all(narrow_up, "shard", split_axis=2, concat_axis=1, tiled=True),
    )
    scale_gate = lax.dynamic_slice_in_dim(
        scale_gate, lax.axis_index("shard") * serve_gate.shape[2], serve_gate.shape[2], axis=1
    )
    scale_up = lax.dynamic_slice_in_dim(
        scale_up, lax.axis_index("shard") * serve_up.shape[2], serve_up.shape[2], axis=1
    )
    part_router = (router_weight * router_gain[:, None]).astype(jnp.bfloat16)
    row_router = lax.all_gather(part_router, "shard", axis=0, tiled=True)
    serve_router = lax.all_gather(row_router, "expert", axis=1, tiled=True)
    return (serve_gate, serve_up, scale_gate, scale_up, serve_router)


def body(n, ne, w_gate, w_up, router_weight, router_gain):
    experts, rows, cols = w_gate.shape
    total, h = 2 * experts, n // 2
    fits = (
        n % 2 == 0 and rows % LANES == 0 and cols % LANES == 0 and (cols // n) % 16 == 0
        and total > DIRECT and (total - DIRECT) % h == 0 and (total - DIRECT) % CHUNK == 0
        and total >= SLOTS and total - SECOND >= max(experts + PLACES, DIRECT + CHUNK)
        and (total - SECOND - DIRECT) % CHUNK == 0 and experts % PLACES == 0
    )
    if not fits:
        return plain_body(w_gate, w_up, router_weight, router_gain)
    part, share, local_e = cols // n, (total - DIRECT) // h, router_weight.shape[1]
    lo, hi = total - SECOND, total - SHORT
    dma = pltpu.SemaphoreType.DMA
    anywhere = pl.BlockSpec(memory_space=pl.ANY)
    local = pl.BlockSpec(memory_space=pltpu.VMEM)
    serve, late, scale, router = pl.pallas_call(
        functools.partial(kernel, n, ne),
        out_shape=(
            pltpu.VMEM((hi, part, n * rows), jnp.bfloat16),
            pltpu.VMEM((SECOND, cols, rows), jnp.bfloat16),
            pltpu.VMEM((total, part), jnp.float32),
            pltpu.VMEM((n * rows, ne * local_e), jnp.bfloat16),
        ),
        in_specs=[anywhere, anywhere, local, local],
        out_specs=(local, local, local, local),
        scratch_shapes=[
            pltpu.VMEM((total, 1, cols), jnp.float32),
            pltpu.VMEM((SLOTS, rows, cols), jnp.float32),
            pltpu.VMEM((NOW, cols, rows), jnp.float32),
            pltpu.VMEM((lo, cols, rows), jnp.bfloat16),
            pltpu.VMEM((total, 1, cols), jnp.float32),
            pltpu.VMEM((n, NOW, 1, cols), jnp.float32),
            pltpu.VMEM((h, DIRECT - NOW, 1, cols), jnp.float32),
            pltpu.VMEM((DIRECT - NOW, 1, cols), jnp.float32),
            pltpu.VMEM((DIRECT - NOW, 1, cols), jnp.float32),
            pltpu.VMEM((h, share, 1, cols), jnp.float32),
            pltpu.VMEM((share, 1, cols), jnp.float32),
            pltpu.VMEM((share, 1, cols), jnp.float32),
            pltpu.VMEM((ne, n, local_e, rows), jnp.bfloat16),
            dma((SLOTS,)),
            dma((n,)),
            dma((n,)),
            dma((n,)),
            dma((n,)),
            dma((h,)),
            dma((h,)),
            dma,
            dma,
            dma((h,)),
            dma((h,)),
            dma,
            dma,
            dma((h,)),
            dma((h,)),
            dma,
            dma,
            dma((h, 2)),
            dma((h, 2)),
            dma((ne,)),
            dma((ne,)),
        ],
        compiler_params=pltpu.CompilerParams(
            collective_id=0, has_side_effects=True, vmem_limit_bytes=30 * 2**20
        ),
        cost_estimate=pl.CostEstimate(
            flops=4 * experts * rows * cols, bytes_accessed=20 * experts * rows * cols, transcendentals=0
        ),
    )(w_gate, w_up, router_weight.T, router_gain[None, :])
    gate, up, scale_gate, scale_up, router, token = pl.pallas_call(
        functools.partial(place, lo),
        out_shape=(
            pltpu.HBM((experts, part, n * rows), jnp.bfloat16),
            pltpu.HBM((experts, part, n * rows), jnp.bfloat16),
            pltpu.HBM((experts, part), jnp.float32),
            pltpu.HBM((experts, part), jnp.float32),
            pltpu.HBM((n * rows, ne * local_e), jnp.bfloat16),
            pltpu.HBM((8, part), jnp.float32),
        ),
        in_specs=[local] * 3,
        out_specs=(anywhere,) * 6,
        scratch_shapes=[dma((2 * PLACES + 4,))],
        compiler_params=pltpu.CompilerParams(vmem_limit_bytes=2**20),
        cost_estimate=pl.CostEstimate(
            flops=0, bytes_accessed=4 * experts * rows * cols, transcendentals=0
        ),
    )(serve, scale, router)
    tail = pl.pallas_call(
        functools.partial(second, n),
        out_shape=pltpu.VMEM((SECOND, part, n * rows), jnp.bfloat16),
        in_specs=[local, anywhere],
        out_specs=local,
        scratch_shapes=[dma((n,)), dma((n,))],
        compiler_params=pltpu.CompilerParams(
            collective_id=1, has_side_effects=True, vmem_limit_bytes=2**20
        ),
        cost_estimate=pl.CostEstimate(
            flops=0, bytes_accessed=SECOND * rows * cols, transcendentals=0
        ),
    )(late, token)
    up = pl.pallas_call(
        functools.partial(place_second, lo),
        out_shape=pltpu.HBM((experts, part, n * rows), jnp.bfloat16),
        in_specs=[local, local, anywhere],
        out_specs=anywhere,
        input_output_aliases={2: 0},
        scratch_shapes=[dma((4,))],
        compiler_params=pltpu.CompilerParams(vmem_limit_bytes=2**20),
        cost_estimate=pl.CostEstimate(
            flops=0, bytes_accessed=4 * SECOND * rows * cols, transcendentals=0
        ),
    )(serve, tail, up)
    return (jnp.swapaxes(gate, 1, 2), jnp.swapaxes(up, 1, 2), scale_gate, scale_up, router)


def solution(mesh):
    return jax.shard_map(
        functools.partial(body, mesh.shape["shard"], mesh.shape["expert"]),
        mesh=mesh,
        in_specs=(
            P("expert", "shard", None),
            P("expert", "shard", None),
            P("shard", "expert"),
            P("shard"),
        ),
        out_specs=(
            P("expert", None, "shard"),
            P("expert", None, "shard"),
            P("expert", "shard"),
            P("expert", "shard"),
            P(),
        ),
        check_vma=False,
    )
```
